128 devices in a mesh: gx: 4 (over z), gy: 8 (over x, core), gz: 4 (over y).
Axes of the slice: x: 4, y: 4, z: 4, core: 2. Of those that a mesh axis runs over, the one named last changes fastest.
Arguments:
- queries: bfloat16 [256, 1024, 512], P(('gx', 'gy'), 'gz'), may hold values from -48 to 48
- key_vectors: bfloat16 [256, 1024, 128], P(('gx', 'gy'), 'gz'), may hold values from -12 to 12
- value_vectors: bfloat16 [256, 1024, 128], P(('gx', 'gy'), 'gz'), may hold values from -6 to 6
- chosen: int32 [256, 2], P(('gx', 'gy')), may hold values from -1 to 255, as said below
Outputs:
- attended: bfloat16 [256, 1024, 512], P(('gx', 'gy'), 'gz')
The draws below stay inside these ranges and needn't reach their ends.
Inputs may be any that keep to these rules, and one draw needn't show every extreme that they name: `chosen`: both entries of a row are -1, or both are blocks of two different groups before the row's own group, counting blocks in groups of 8 consecutive blocks. One group's rows name blocks of any one group in at most 1 entries; every group from the third on names blocks of the first group in exactly 1 entries. The rows of the first two groups are all -1.
All inputs are finite; a program needn't handle non-finite values.
Results may differ from the reference program's by a relative error of at most 0.0042.
Values may be sent and summed in bfloat16 or wider, within the bound.
A program may use at most 128 MiB of HBM per device.

```python
import jax
import jax.numpy as jnp
from jax import lax

DH = 128
GROUP = 4
BLK = 1024
BG = 8
NBLK = 256


def draw_key_vectors(key, part):
    base_key = jax.random.fold_in(key, 202)
    base_draw = jnp.clip(jax.random.normal(base_key, (NBLK, BLK, DH), jnp.float32), -4.0, 4.0)
    return base_draw.astype(jnp.bfloat16)


def draw_queries(key, part):
    base_key = jax.random.fold_in(key, 303)
    base_draw = jnp.clip(jax.random.normal(base_key, (NBLK, BLK, GROUP * DH), jnp.float32), -4.0, 4.0)
    return base_draw.astype(jnp.bfloat16)


def draw_chosen(key, part):
    groups = NBLK // BG
    slot_count = 2 * BG
    perm_key, block_key = jax.random.split(jax.random.fold_in(key, 404), 2)
    shuffled = jax.vmap(lambda single: jax.random.permutation(single, groups))(jax.random.split(perm_key, groups)).astype(jnp.int32)
    group_ids = jnp.arange(groups, dtype=jnp.int32)[:, None]
    usable = (shuffled >= 1) & (shuffled < group_ids)
    order_score = jnp.where(usable, 0, groups) + jnp.arange(groups, dtype=jnp.int32)[None, :]
    ordering = jnp.argsort(order_score, axis=1)
    picked = jnp.take_along_axis(shuffled, ordering, axis=1)
    picked_ok = jnp.take_along_axis(usable, ordering, axis=1)
    padding = jnp.zeros((groups, slot_count), jnp.int32)
    picked = jnp.concatenate([picked, padding], axis=1)[:, :slot_count - 1]
    picked_ok = jnp.concatenate([picked_ok, padding > 0], axis=1)[:, :slot_count - 1]
    owner_group = jnp.concatenate([jnp.zeros((groups, 1), jnp.int32), picked], axis=1)
    owner_ok = jnp.concatenate([group_ids >= 1, picked_ok], axis=1)
    inner_pick = jax.random.randint(block_key, (groups, slot_count), 0, BG).astype(jnp.int32)
    entries = (owner_group * BG + inner_pick).reshape(groups, BG, 2)
    row_live = owner_ok.reshape(groups, BG, 2)[:, :, 1:2]
    pair = jnp.where(row_live, entries, -1)
    return pair.reshape(NBLK, 2).astype(jnp.int32)


def block_scale(own_key, dims, pieces, smallest, high):
    factor_of = 1.0
    for dim, blocks in pieces:
        draws = jax.random.uniform(jax.random.fold_in(jax.random.fold_in(own_key, 6), dim), (blocks,), jnp.float32, smallest / len(pieces), high / len(pieces))
        factor_of = factor_of * jnp.repeat(jnp.exp(draws), dims[dim] // blocks).reshape((-1,) + (1,) * (len(dims) - 1 - dim))
    return factor_of


def bell_draw(stream_key, dims, spread, reach, cuts=(), kind=jnp.bfloat16):
    values = spread * jax.random.normal(stream_key, dims, jnp.float32)
    if cuts:
        values = values * block_scale(stream_key, dims, cuts, -0.22, 0.18)
    return jnp.clip(values, -reach, reach).astype(kind)


def setup_inputs(seed: int = 0) -> dict:
    streams_of = jax.random.split(jax.random.key(seed), 5)
    queries = draw_queries(jax.random.fold_in(streams_of[4], 71), 0)
    key_vectors = draw_key_vectors(jax.random.fold_in(streams_of[4], 71), 0)
    value_vectors = bell_draw(streams_of[2], (NBLK, BLK, DH), 1.0, 6.0, ((0, 32), (1, 4)))
    chosen = draw_chosen(jax.random.fold_in(streams_of[4], 71), 0)
    return {"queries": queries, "key_vectors": key_vectors, "value_vectors": value_vectors, "chosen": chosen}


def allowed_mask(token_start, query_count, head_count, block_len, live_pair):
    token_pos = token_start + jnp.arange(query_count * head_count, dtype=jnp.int32) // head_count
    key_pos = jnp.arange(3 * block_len, dtype=jnp.int32)
    own_part = (key_pos[None, :] < block_len) & (key_pos[None, :] <= token_pos[:, None])
    pair_slot = jnp.clip(key_pos // block_len - 1, 0, 1)
    far_part = (key_pos >= block_len) & (live_pair[pair_slot] > 0)
    return own_part | far_part[None, :]


def attend_block(query_block, key_sets, value_sets, allowed):
    head_dim = key_sets.shape[1]
    flat_queries = query_block.reshape(-1, head_dim)
    scores = jnp.dot(flat_queries, key_sets.T, preferred_element_type=jnp.float32) * (head_dim ** -0.5)
    scores = jnp.where(allowed, scores, -jnp.inf)
    row_top = jnp.max(scores, axis=1, keepdims=True)
    weights = jnp.exp(scores - row_top)
    row_total = jnp.sum(weights, axis=1, keepdims=True)
    mixed = jnp.dot(weights.astype(jnp.bfloat16), value_sets, preferred_element_type=jnp.float32) / row_total
    return mixed.astype(jnp.bfloat16).reshape(query_block.shape)


def reference(queries, key_vectors, value_vectors, chosen):
    block_len = key_vectors.shape[1]
    head_dim = key_vectors.shape[2]
    head_count = queries.shape[2] // head_dim

    def one_block(block_index):
        picked_pair = chosen[block_index]
        live_pair = (picked_pair >= 0).astype(jnp.int32)
        safe_picks = jnp.maximum(picked_pair, 0)
        key_sets = jnp.concatenate([key_vectors[block_index], key_vectors[safe_picks[0]], key_vectors[safe_picks[1]]], axis=0)
        value_sets = jnp.concatenate([value_vectors[block_index], value_vectors[safe_picks[0]], value_vectors[safe_picks[1]]], axis=0)
        allowed = allowed_mask(0, block_len, head_count, block_len, live_pair)
        return attend_block(queries[block_index], key_sets, value_sets, allowed)

    return lax.map(one_block, jnp.arange(NBLK, dtype=jnp.int32))
```

```python
import functools

import jax
import jax.numpy as jnp
from jax import lax
from jax.experimental import pallas as pl
from jax.experimental.pallas import tpu as pltpu
from jax.sharding import PartitionSpec as P

MESH = pl.DeviceIdType.MESH
STAGES = (64, 64, 64, 64)
AHEAD = 2
PAIR = 2
NEG = -1e30
LOG2E = 1.4426950408889634


def kernel(dims, ch, q_hbm, k_hbm, v_hbm, out_hbm, *scratch):
    NX, NY, NZ, HEADS, DH, QT, ROWS = dims
    NG = NX * NY
    S = len(STAGES)
    STARTS = [sum(STAGES[:s]) for s in range(S)]
    BLOCKS = NZ * ROWS
    qb, okv, want, rqv, rqs, m_s, l_s, acc, obuf = scratch[:9]
    kv_sem, self_sem, y_send, y_recv, w_send, w_recv, rq_sem = scratch[9:16]
    a_send, a_recv, f_send, f_recv, o_send, o_recv = scratch[16:22]
    stg, recv, kvb, sel, far = (scratch[22 + S * n : 22 + S * (n + 1)] for n in range(5))

    gx, gy, gz = lax.axis_index("gx"), lax.axis_index("gy"), lax.axis_index("gz")
    g = gx * NY + gy
    xx, cc = gy // 2, lax.rem(gy, 2)
    NXX = NY // 2

    def plane(t):
        return (t // NY, lax.rem(t, NY), gz)

    def line(d):
        return lax.rem(gz + d, NZ)

    loads = []
    for s in range(S):
        for c, src in enumerate((k_hbm, v_hbm)):
            loads.append(
                pltpu.make_async_copy(
                    src.at[:, pl.ds(STARTS[s], STAGES[s])], kvb[s].at[:, c], kv_sem.at[2 * s + c]
                )
            )
    mine = pl.ds(ROWS * gz, ROWS)
    selfs = [
        pltpu.make_async_copy(k_hbm.at[mine], okv.at[:, gz, 0], self_sem.at[0]),
        pltpu.make_async_copy(v_hbm.at[mine], okv.at[:, gz, 1], self_sem.at[1]),
        pltpu.make_async_copy(q_hbm.at[mine], qb.at[:, gz], self_sem.at[2]),
    ]
    for cp in loads + selfs:
        cp.start()

    rqv[...] = jnp.zeros((NG, 1, 128), jnp.int32)

    bar = pltpu.get_barrier_semaphore()

    @pl.loop(1, NG)
    def _(s):
        pl.semaphore_signal(
            bar, 1, device_id=plane(lax.rem(g + s, NG)), device_id_type=MESH
        )

    for d in range(1, NZ):
        pl.semaphore_signal(bar, 1, device_id=(gx, gy, line(d)), device_id_type=MESH)

    owner_row = lax.broadcasted_iota(jnp.int32, (NG, 1, 128), 0)
    table = jnp.zeros((NG, 1, 128), jnp.int32)
    for b in range(BLOCKS):
        for j in range(2):
            e = ch[j, b]
            live = e >= 0
            o = jnp.where(live, lax.shift_right_logical(e, 3), -1)
            table = jnp.where(owner_row == o, lax.bitwise_and(e, 7) + 1, table)
    want[...] = table
    pl.semaphore_wait(bar, NG - 1 + NZ - 1)

    def ask(t, slot):
        return pltpu.make_async_remote_copy(
            src_ref=want.at[t], dst_ref=rqv.at[slot], send_sem=w_send.at[t],
            recv_sem=w_recv.at[slot], device_id=plane(t), device_id_type=MESH,
        )

    def sends_to(t):
        return (t > g) & (t >= 2)

    def gets_from(t):
        return (t < g) & (g >= 2)

    @pl.loop(0, NG)
    def _(t):
        @pl.when(gets_from(t))
        def _():
            ask(t, g).start()

    def ycopies(r, d):
        row, z, src_z = ROWS * line(d) + r, line(d), gz
        out = []
        for n, (src, dst) in enumerate(
            (
                (k_hbm.at[row], okv.at[r, src_z, 0]),
                (v_hbm.at[row], okv.at[r, src_z, 1]),
                (q_hbm.at[row], qb.at[r, src_z]),
            )
        ):
            out.append(
                pltpu.make_async_remote_copy(
                    src_ref=src, dst_ref=dst, send_sem=y_send.at[r, d - 1, n],
                    recv_sem=y_recv.at[r, d - 1, n], device_id=(gx, gy, z), device_id_type=MESH,
                )
            )
        return out

    DORDER = (1, 3, 2)
    for r in range(ROWS):
        for d in DORDER:
            for cp in ycopies(r, d):
                cp.start()

    for cp in loads:
        cp.wait()

    @pl.loop(0, NG)
    def _(t):
        @pl.when(sends_to(t))
        def _():
            ask(t, t).wait_recv()

        @pl.when(gets_from(t))
        def _():
            ask(t, g).wait_send()

    rq = pltpu.make_async_copy(rqv, rqs, rq_sem)
    rq.start()
    rq.wait()

    def give(s, t, slot):
        return pltpu.make_async_remote_copy(
            src_ref=stg[s].at[t], dst_ref=recv[s].at[slot], send_sem=a_send.at[s, t],
            recv_sem=a_recv.at[s, slot], device_id=plane(t), device_id_type=MESH,
        )

    def shifted(dz, dx, dc):
        return (
            lax.rem(gx + dz, NX) * NY + lax.rem(xx + dx, NXX) * 2 + lax.rem(cc + dc, 2)
        )

    def stage(s):
        @pl.loop(0, NG)
        def _(t):
            @pl.when(sends_to(t))
            def _():
                idx = jnp.maximum(rqs[t, 0, 0] - 1, 0)
                stg[s][t] = kvb[s][idx]

        recv[s][g] = kvb[s][0]

    def fire(s):
        def one(t):
            @pl.when(sends_to(t))
            def _():
                give(s, t, g).start()

        @pl.loop(0, 8)
        def _(i):
            one(shifted(i // 2, 2, lax.rem(i, 2)))

        @pl.loop(0, 16)
        def _(i):
            one(shifted(i // 4, 1 + 2 * lax.rem(i // 2, 2), lax.rem(i, 2)))

        @pl.loop(1, 8)
        def _(i):
            one(shifted(i // 2, 0, lax.rem(i, 2)))

    for s in range(S):
        stage(s)
        if s < AHEAD:
            fire(s)

    c2 = DH ** -0.5 * LOG2E

    def heads_of(r, qq, h):
        return qb[r, qq, :, h * DH : (h + 1) * DH]

    def scores_of(r, qq, h, keys):
        return lax.dot_general(
            heads_of(r, qq, h), keys, (((1,), (1,)), ((), ())),
            preferred_element_type=jnp.float32,
        )

    def weigh(p, values):
        ones = jnp.ones(values.shape, jnp.bfloat16)
        both = jnp.dot(
            p.astype(jnp.bfloat16), jnp.concatenate([values, ones], axis=1),
            preferred_element_type=jnp.float32,
        )
        return both[:, :DH], both[:, DH:]

    tok = lax.broadcasted_iota(jnp.int32, (QT, QT), 0)
    key_pos = lax.broadcasted_iota(jnp.int32, (QT, QT), 1)
    diag = key_pos <= tok

    def wide(x, n):
        return jnp.concatenate([x] * (n // DH), axis=1) if n > DH else x

    def pipeline(items):
        ready = items[0][0]()
        for n, (_, finish) in enumerate(items):
            ahead = items[n + 1][0]() if n + 1 < len(items) else None
            finish(ready)
            ready = ahead

    def peak(sc):
        return jnp.broadcast_to(jnp.max(sc, axis=1, keepdims=True), (QT, DH))

    def own_item(r, qq, h):
        n = qq + 1

        def first():
            return scores_of(r, qq, h, okv[r, 0:n, 0].reshape(n * QT, DH))

        def finish(sc):
            last = jnp.where(diag, sc[:, qq * QT :], NEG)
            sc = jnp.concatenate([sc[:, : qq * QT], last], axis=1) if qq else last
            top = peak(sc)
            p = jnp.exp2(sc * c2 - wide(top * c2, n * QT))
            pv, tot = weigh(p, okv[r, 0:n, 1].reshape(n * QT, DH))
            m_s[r, qq, h] = top
            l_s[r, qq, h] = tot
            acc[r, qq, h] = pv

        return first, finish

    def own(r):
        pipeline([own_item(r, qq, h) for qq in range(NZ) for h in range(HEADS)])

    def far_item(s, r, qq, h, live, last):
        n = 2 * NZ * STAGES[s]

        def first():
            return scores_of(r, qq, h, far[s][r, :, :, 0].reshape(n, DH))

        def finish(sc):
            old = m_s[r, qq, h]
            new = jnp.where(live, jnp.maximum(old, peak(sc)), old)
            base = jnp.where(live, new * c2, -NEG)
            p = jnp.exp2(sc * c2 - wide(base, n))
            fade = jnp.exp2((old - new) * c2)
            pv, tot = weigh(p, far[s][r, :, :, 1].reshape(n, DH))
            a_new = acc[r, qq, h] * fade + pv
            l_new = l_s[r, qq, h] * fade + tot
            if last:
                obuf[r, qq, :, h * DH : (h + 1) * DH] = (a_new / l_new).astype(jnp.bfloat16)
            else:
                m_s[r, qq, h] = new
                acc[r, qq, h] = a_new
                l_s[r, qq, h] = l_new

        return first, finish

    def extend(s, r, qqs, last):
        live = ch[0, ROWS * gz + r] >= 0
        pipeline([far_item(s, r, qq, h, live, last) for qq in qqs for h in range(HEADS)])

    def fcopy(s, r, d):
        return pltpu.make_async_remote_copy(
            src_ref=sel[s].at[r, d - 1], dst_ref=far[s].at[r, gz],
            send_sem=f_send.at[s, r, d - 1], recv_sem=f_recv.at[s, r, d - 1],
            device_id=(gx, gy, line(d)), device_id_type=MESH,
        )

    def forward(s):
        @pl.loop(0, NG)
        def _(t):
            @pl.when(gets_from(t))
            def _():
                give(s, t, t).wait_recv()

        if s + AHEAD < S:
            fire(s + AHEAD)

        for r in range(ROWS):
            for d in DORDER + (NZ,):
                for j in range(2):
                    e = ch[j, ROWS * line(d) + r]
                    o = jnp.where(e >= 0, lax.shift_right_logical(e, 3), g)
                    val = recv[s][o]
                    if d < NZ:
                        sel[s][r, d - 1, j] = val
                    else:
                        far[s][r, gz, j] = val
            for d in DORDER:
                fcopy(s, r, d).start()

    def wait_own(r):
        for d in DORDER:
            for cp in ycopies(r, d):
                cp.wait_recv()

    def wait_far(s, r):
        for d in DORDER:
            fcopy(s, r, d).wait_recv()

    for cp in selfs:
        cp.wait()
    wait_own(0)
    own(0)
    forward(0)
    wait_own(1)
    own(1)
    if S > 1:
        forward(1)
    for s in range(S - 1):
        for r in range(ROWS):
            wait_far(s, r)

            @pl.loop(0, NZ // PAIR)
            def _(i, s=s, r=r):
                extend(s, r, [PAIR * i + n for n in range(PAIR)], False)

        if s + 2 < S:
            forward(s + 2)

    def ocopy(r, d):
        return pltpu.make_async_remote_copy(
            src_ref=obuf.at[r, line(d)], dst_ref=out_hbm.at[ROWS * gz + r],
            send_sem=o_send.at[r, d - 1], recv_sem=o_recv.at[r, d - 1],
            device_id=(gx, gy, line(d)), device_id_type=MESH,
        )

    def olocal(r):
        return pltpu.make_async_copy(
            obuf.at[r, gz], out_hbm.at[ROWS * gz + r], o_send.at[r, NZ - 1]
        )

    for r in range(ROWS):
        wait_far(S - 1, r)

        @pl.loop(1, NZ + 1)
        def _(d, r=r):
            extend(S - 1, r, [lax.rem(gz + d, NZ)], True)

            @pl.when(d >= 2)
            def _():
                ocopy(r, d - 1).start()

        olocal(r).start()

    for r in range(ROWS):
        for d in range(1, NZ):
            for cp in ycopies(r, d):
                cp.wait_send()
            for s in range(S):
                fcopy(s, r, d).wait_send()
    for s in range(S):

        @pl.loop(0, NG)
        def _(t, s=s):
            @pl.when(sends_to(t))
            def _():
                give(s, t, g).wait_send()

    for r in range(ROWS):
        for d in range(1, NZ):
            ocopy(r, d).wait()
        olocal(r).wait()


def body(queries, key_vectors, value_vectors, chosen):
    blocks, quarter, width = queries.shape
    dh = key_vectors.shape[2]
    heads = width // dh
    nx, ny, nz = (lax.axis_size(a) for a in ("gx", "gy", "gz"))
    rows = blocks // nz
    ng = nx * ny
    s = len(STAGES)
    bf, f32, i32 = jnp.bfloat16, jnp.float32, jnp.int32
    dma = pltpu.SemaphoreType.DMA
    scratch = [
        pltpu.VMEM((rows, nz, quarter, width), bf),
        pltpu.VMEM((rows, nz, 2, quarter, dh), bf),
        pltpu.VMEM((ng, 1, 128), i32),
        pltpu.VMEM((ng, 1, 128), i32),
        pltpu.SMEM((ng, 1, 128), i32),
        pltpu.VMEM((rows, nz, heads, quarter, dh), f32),
        pltpu.VMEM((rows, nz, heads, quarter, dh), f32),
        pltpu.VMEM((rows, nz, heads, quarter, dh), f32),
        pltpu.VMEM((rows, nz, quarter, width), bf),
        dma((2 * s,)),
        dma((3,)),
        dma((rows, nz - 1, 3)),
        dma((rows, nz - 1, 3)),
        dma((ng,)),
        dma((ng,)),
        dma,
        dma((s, ng)),
        dma((s, ng)),
        dma((s, rows, nz - 1)),
        dma((s, rows, nz - 1)),
        dma((rows, nz)),
        dma((rows, nz)),
    ]
    for lead in ((ng,), (ng,), (blocks,), (rows, nz - 1, 2), (rows, nz, 2)):
        scratch += [pltpu.VMEM(lead + (2, t, dh), bf) for t in STAGES]
    return pl.pallas_call(
        functools.partial(kernel, (nx, ny, nz, heads, dh, quarter, rows)),
        out_shape=jax.ShapeDtypeStruct(queries.shape, bf),
        in_specs=[pl.BlockSpec(memory_space=pltpu.SMEM)]
        + [pl.BlockSpec(memory_space=pl.ANY)] * 3,
        out_specs=pl.BlockSpec(memory_space=pl.ANY),
        scratch_shapes=scratch,
        compiler_params=pltpu.CompilerParams(
            collective_id=0, has_side_effects=True, vmem_limit_bytes=60 * 1024 * 1024
        ),
    )(chosen.T, queries, key_vectors, value_vectors)


def solution(mesh):
    placed = (
        P(("gx", "gy"), "gz", None),
        P(("gx", "gy"), "gz", None),
        P(("gx", "gy"), "gz", None),
        P(("gx", "gy"), None),
    )
    return jax.shard_map(
        body, mesh=mesh, in_specs=placed, out_specs=P(("gx", "gy"), "gz", None), check_vma=False
    )
```

```python
import functools

import jax
import jax.numpy as jnp
from jax import lax
from jax.experimental import pallas as pl
from jax.experimental.pallas import tpu as pltpu
from jax.sharding import PartitionSpec as P

MESH = pl.DeviceIdType.MESH
STAGES = (64, 64, 64, 64)
AHEAD = 2
PAIR = 2
NEG = -1e30
LOG2E = 1.4426950408889634


def kernel(dims, ch, q_hbm, k_hbm, v_hbm, out_ref, *scratch):
    NX, NY, NZ, HEADS, DH, QT, ROWS = dims
    NG = NX * NY
    S = len(STAGES)
    STARTS = [sum(STAGES[:s]) for s in range(S)]
    BLOCKS = NZ * ROWS
    qb, okv, want, rqv, rqs, m_s, l_s, acc, obuf = scratch[:9]
    kv_sem, self_sem, y_send, y_recv, w_send, w_recv, rq_sem = scratch[9:16]
    a_send, a_recv, f_send, f_recv, o_send, o_recv = scratch[16:22]
    stg, recv, kvb, sel, far = (scratch[22 + S * n : 22 + S * (n + 1)] for n in range(5))

    gx, gy, gz = lax.axis_index("gx"), lax.axis_index("gy"), lax.axis_index("gz")
    g = gx * NY + gy
    xx, cc = gy // 2, lax.rem(gy, 2)
    NXX = NY // 2

    def plane(t):
        return (t // NY, lax.rem(t, NY), gz)

    def line(d):
        return lax.rem(gz + d, NZ)

    loads = []
    for s in range(S):
        for c, src in enumerate((k_hbm, v_hbm)):
            loads.append(
                pltpu.make_async_copy(
                    src.at[:, pl.ds(STARTS[s], STAGES[s])], kvb[s].at[:, c], kv_sem.at[2 * s + c]
                )
            )
    mine = pl.ds(ROWS * gz, ROWS)
    selfs = [
        pltpu.make_async_copy(k_hbm.at[mine], okv.at[:, gz, 0], self_sem.at[0]),
        pltpu.make_async_copy(v_hbm.at[mine], okv.at[:, gz, 1], self_sem.at[1]),
        pltpu.make_async_copy(q_hbm.at[mine], qb.at[:, gz], self_sem.at[2]),
    ]
    for cp in loads + selfs:
        cp.start()

    rqv[...] = jnp.zeros((NG, 1, 128), jnp.int32)

    bar = pltpu.get_barrier_semaphore()

    @pl.loop(1, NG)
    def _(s):
        pl.semaphore_signal(
            bar, 1, device_id=plane(lax.rem(g + s, NG)), device_id_type=MESH
        )

    for d in range(1, NZ):
        pl.semaphore_signal(bar, 1, device_id=(gx, gy, line(d)), device_id_type=MESH)

    owner_row = lax.broadcasted_iota(jnp.int32, (NG, 1, 128), 0)
    table = jnp.zeros((NG, 1, 128), jnp.int32)
    for b in range(BLOCKS):
        for j in range(2):
            e = ch[j, b]
            live = e >= 0
            o = jnp.where(live, lax.shift_right_logical(e, 3), -1)
            table = jnp.where(owner_row == o, lax.bitwise_and(e, 7) + 1, table)
    want[...] = table
    pl.semaphore_wait(bar, NG - 1 + NZ - 1)

    def ask(t, slot):
        return pltpu.make_async_remote_copy(
            src_ref=want.at[t], dst_ref=rqv.at[slot], send_sem=w_send.at[t],
            recv_sem=w_recv.at[slot], device_id=plane(t), device_id_type=MESH,
        )

    def sends_to(t):
        return (t > g) & (t >= 2)

    def gets_from(t):
        return (t < g) & (g >= 2)

    @pl.loop(0, NG)
    def _(t):
        @pl.when(gets_from(t))
        def _():
            ask(t, g).start()

    def ycopies(r, d):
        row, z, src_z = ROWS * line(d) + r, line(d), gz
        out = []
        for n, (src, dst) in enumerate(
            (
                (k_hbm.at[row], okv.at[r, src_z, 0]),
                (v_hbm.at[row], okv.at[r, src_z, 1]),
                (q_hbm.at[row], qb.at[r, src_z]),
            )
        ):
            out.append(
                pltpu.make_async_remote_copy(
                    src_ref=src, dst_ref=dst, send_sem=y_send.at[r, d - 1, n],
                    recv_sem=y_recv.at[r, d - 1, n], device_id=(gx, gy, z), device_id_type=MESH,
                )
            )
        return out

    DORDER = (1, 3, 2)
    for r in range(ROWS):
        for d in DORDER:
            for cp in ycopies(r, d):
                cp.start()

    for cp in loads:
        cp.wait()

    @pl.loop(0, NG)
    def _(t):
        @pl.when(sends_to(t))
        def _():
            ask(t, t).wait_recv()

    rq = pltpu.make_async_copy(rqv, rqs, rq_sem)
    rq.start()
    rq.wait()

    def give(s, t, slot):
        return pltpu.make_async_remote_copy(
            src_ref=stg[s].at[t], dst_ref=recv[s].at[slot], send_sem=a_send.at[s, t],
            recv_sem=a_recv.at[s, slot], device_id=plane(t), device_id_type=MESH,
        )

    def shifted(dz, dx, dc):
        return (
            lax.rem(gx + dz, NX) * NY + lax.rem(xx + dx, NXX) * 2 + lax.rem(cc + dc, 2)
        )

    def stage(s):
        @pl.loop(0, NG)
        def _(t):
            @pl.when(sends_to(t))
            def _():
                idx = jnp.maximum(rqs[t, 0, 0] - 1, 0)
                stg[s][t] = kvb[s][idx]

        recv[s][g] = kvb[s][0]

    def fire(s):
        def one(t):
            @pl.when(sends_to(t))
            def _():
                give(s, t, g).start()

        @pl.loop(0, 8)
        def _(i):
            one(shifted(i // 2, 2, lax.rem(i, 2)))

        @pl.loop(0, 16)
        def _(i):
            one(shifted(i // 4, 1 + 2 * lax.rem(i // 2, 2), lax.rem(i, 2)))

        @pl.loop(1, 8)
        def _(i):
            one(shifted(i // 2, 0, lax.rem(i, 2)))

    for s in range(S):
        stage(s)
        if s < AHEAD:
            fire(s)

    c2 = DH ** -0.5 * LOG2E

    def heads_of(r, qq, h):
        return qb[r, qq, :, h * DH : (h + 1) * DH]

    def scores_of(r, qq, h, keys):
        return lax.dot_general(
            heads_of(r, qq, h), keys, (((1,), (1,)), ((), ())),
            preferred_element_type=jnp.float32,
        )

    def weigh(p, values):
        ones = jnp.ones(values.shape, jnp.bfloat16)
        both = jnp.dot(
            p.astype(jnp.bfloat16), jnp.concatenate([values, ones], axis=1),
            preferred_element_type=jnp.float32,
        )
        return both[:, :DH], both[:, DH:]

    tok = lax.broadcasted_iota(jnp.int32, (QT, QT), 0)
    key_pos = lax.broadcasted_iota(jnp.int32, (QT, QT), 1)
    diag = key_pos <= tok

    def wide(x, n):
        return jnp.concatenate([x] * (n // DH), axis=1) if n > DH else x

    def pipeline(items):
        ready = items[0][0]()
        for n, (_, finish) in enumerate(items):
            ahead = items[n + 1][0]() if n + 1 < len(items) else None
            finish(ready)
            ready = ahead

    def peak(sc):
        return jnp.broadcast_to(jnp.max(sc, axis=1, keepdims=True), (QT, DH))

    def own_item(r, qq, h):
        n = qq + 1

        def first():
            return scores_of(r, qq, h, okv[r, 0:n, 0].reshape(n * QT, DH))

        def finish(sc):
            last = jnp.where(diag, sc[:, qq * QT :], NEG)
            sc = jnp.concatenate([sc[:, : qq * QT], last], axis=1) if qq else last
            top = peak(sc)
            p = jnp.exp2(sc * c2 - wide(top * c2, n * QT))
            pv, tot = weigh(p, okv[r, 0:n, 1].reshape(n * QT, DH))
            m_s[r, qq, h] = top
            l_s[r, qq, h] = tot
            acc[r, qq, h] = pv

        return first, finish

    def own(r):
        pipeline([own_item(r, qq, h) for qq in range(NZ) for h in range(HEADS)])

    def far_item(s, r, qq, h, live, last):
        n = 2 * NZ * STAGES[s]

        def first():
            return scores_of(r, qq, h, far[s][r, :, :, 0].reshape(n, DH))

        def finish(sc):
            old = m_s[r, qq, h]
            new = jnp.where(live, jnp.maximum(old, peak(sc)), old)
            base = jnp.where(live, new * c2, -NEG)
            p = jnp.exp2(sc * c2 - wide(base, n))
            fade = jnp.exp2((old - new) * c2)
            pv, tot = weigh(p, far[s][r, :, :, 1].reshape(n, DH))
            a_new = acc[r, qq, h] * fade + pv
            l_new = l_s[r, qq, h] * fade + tot
            if last:
                obuf[r, qq, :, h * DH : (h + 1) * DH] = (a_new / l_new).astype(jnp.bfloat16)
            else:
                m_s[r, qq, h] = new
                acc[r, qq, h] = a_new
                l_s[r, qq, h] = l_new

        return first, finish

    def extend(s, r, qqs, last):
        live = ch[0, ROWS * gz + r] >= 0
        pipeline([far_item(s, r, qq, h, live, last) for qq in qqs for h in range(HEADS)])

    def fcopy(s, r, d):
        return pltpu.make_async_remote_copy(
            src_ref=sel[s].at[r, d - 1], dst_ref=far[s].at[r, gz],
            send_sem=f_send.at[s, r, d - 1], recv_sem=f_recv.at[s, r, d - 1],
            device_id=(gx, gy, line(d)), device_id_type=MESH,
        )

    def forward(s):
        @pl.loop(0, NG)
        def _(t):
            @pl.when(gets_from(t))
            def _():
                give(s, t, t).wait_recv()

        if s + AHEAD < S:
            fire(s + AHEAD)

        for r in range(ROWS):
            for d in DORDER + (NZ,):
                for j in range(2):
                    e = ch[j, ROWS * line(d) + r]
                    o = jnp.where(e >= 0, lax.shift_right_logical(e, 3), g)
                    val = recv[s][o]
                    if d < NZ:
                        sel[s][r, d - 1, j] = val
                    else:
                        far[s][r, gz, j] = val
            for d in DORDER:
                fcopy(s, r, d).start()

    def wait_own(r):
        for d in DORDER:
            for cp in ycopies(r, d):
                cp.wait_recv()

    def wait_far(s, r):
        for d in DORDER:
            fcopy(s, r, d).wait_recv()

    for cp in selfs:
        cp.wait()
    wait_own(0)
    own(0)
    forward(0)
    wait_own(1)
    own(1)
    if S > 1:
        forward(1)
    for s in range(S - 1):
        for r in range(ROWS):
            wait_far(s, r)

            @pl.loop(0, NZ // PAIR)
            def _(i, s=s, r=r):
                extend(s, r, [PAIR * i + n for n in range(PAIR)], False)

        if s + 2 < S:
            forward(s + 2)

    def ocopy(r, d):
        return pltpu.make_async_remote_copy(
            src_ref=obuf.at[r, line(d)], dst_ref=out_ref.at[ROWS * gz + r],
            send_sem=o_send.at[r, d - 1], recv_sem=o_recv.at[r, d - 1],
            device_id=(gx, gy, line(d)), device_id_type=MESH,
        )

    for r in range(ROWS):
        wait_far(S - 1, r)

        @pl.loop(1, NZ + 1)
        def _(d, r=r):
            extend(S - 1, r, [lax.rem(gz + d, NZ)], True)

            @pl.when(d >= 2)
            def _():
                ocopy(r, d - 1).start()

        out_ref[ROWS * gz + r] = obuf[r, gz]

    @pl.loop(0, NG)
    def _(t):
        @pl.when(gets_from(t))
        def _():
            ask(t, g).wait_send()

    for r in range(ROWS):
        for d in range(1, NZ):
            for cp in ycopies(r, d):
                cp.wait_send()
            for s in range(S):
                fcopy(s, r, d).wait_send()
    for s in range(S):

        @pl.loop(0, NG)
        def _(t, s=s):
            @pl.when(sends_to(t))
            def _():
                give(s, t, g).wait_send()

    for r in range(ROWS):
        for d in range(1, NZ):
            ocopy(r, d).wait()


def body(queries, key_vectors, value_vectors, chosen):
    blocks, quarter, width = queries.shape
    dh = key_vectors.shape[2]
    heads = width // dh
    nx, ny, nz = (lax.axis_size(a) for a in ("gx", "gy", "gz"))
    rows = blocks // nz
    ng = nx * ny
    s = len(STAGES)
    bf, f32, i32 = jnp.bfloat16, jnp.float32, jnp.int32
    dma = pltpu.SemaphoreType.DMA
    scratch = [
        pltpu.VMEM((rows, nz, quarter, width), bf),
        pltpu.VMEM((rows, nz, 2, quarter, dh), bf),
        pltpu.VMEM((ng, 1, 128), i32),
        pltpu.VMEM((ng, 1, 128), i32),
        pltpu.SMEM((ng, 1, 128), i32),
        pltpu.VMEM((rows, nz, heads, quarter, dh), f32),
        pltpu.VMEM((rows, nz, heads, quarter, dh), f32),
        pltpu.VMEM((rows, nz, heads, quarter, dh), f32),
        pltpu.VMEM((rows, nz, quarter, width), bf),
        dma((2 * s,)),
        dma((3,)),
        dma((rows, nz - 1, 3)),
        dma((rows, nz - 1, 3)),
        dma((ng,)),
        dma((ng,)),
        dma,
        dma((s, ng)),
        dma((s, ng)),
        dma((s, rows, nz - 1)),
        dma((s, rows, nz - 1)),
        dma((rows, nz - 1)),
        dma((rows, nz - 1)),
    ]
    for lead in ((ng,), (ng,), (blocks,), (rows, nz - 1, 2), (rows, nz, 2)):
        scratch += [pltpu.VMEM(lead + (2, t, dh), bf) for t in STAGES]
    return pl.pallas_call(
        functools.partial(kernel, (nx, ny, nz, heads, dh, quarter, rows)),
        out_shape=pltpu.VMEM(queries.shape, bf),
        in_specs=[pl.BlockSpec(memory_space=pltpu.SMEM)]
        + [pl.BlockSpec(memory_space=pltpu.HBM)] * 3,
        out_specs=pl.BlockSpec(memory_space=pltpu.VMEM),
        scratch_shapes=scratch,
        compiler_params=pltpu.CompilerParams(
            collective_id=0, has_side_effects=True, vmem_limit_bytes=67043328 - 9 * 262144
        ),
    )(chosen.T, queries, key_vectors, value_vectors)


def solution(mesh):
    placed = (
        P(("gx", "gy"), "gz", None),
        P(("gx", "gy"), "gz", None),
        P(("gx", "gy"), "gz", None),
        P(("gx", "gy"), None),
    )
    return jax.shard_map(
        body, mesh=mesh, in_specs=placed, out_specs=P(("gx", "gy"), "gz", None), check_vma=False
    )
```

```python
import functools

import jax
import jax.numpy as jnp
from jax import lax
from jax.experimental import pallas as pl
from jax.experimental.pallas import tpu as pltpu
from jax.sharding import PartitionSpec as P

MESH = pl.DeviceIdType.MESH
STAGES = (64, 64, 64, 64)
AHEAD = 2
PAIR = 2
NEG = -1e30
LOG2E = 1.4426950408889634


def kernel(dims, ch, q_hbm, k_hbm, v_hbm, out_ref, *scratch):
    NX, NY, NZ, HEADS, DH, QT, ROWS = dims
    NG = NX * NY
    S = len(STAGES)
    STARTS = [sum(STAGES[:s]) for s in range(S)]
    BLOCKS = NZ * ROWS
    qb, okv, want, rqv, rqs, m_s, l_s, acc, obuf = scratch[:9]
    kv_sem, self_sem, y_send, y_recv, w_send, w_recv, rq_sem = scratch[9:16]
    a_send, a_recv, f_send, f_recv, o_send, o_recv = scratch[16:22]
    stg, recv, kvb, sel, far = (scratch[22 + S * n : 22 + S * (n + 1)] for n in range(5))

    gx, gy, gz = lax.axis_index("gx"), lax.axis_index("gy"), lax.axis_index("gz")
    g = gx * NY + gy
    xx, cc = gy // 2, lax.rem(gy, 2)
    NXX = NY // 2

    def plane(t):
        return (t // NY, lax.rem(t, NY), gz)

    def line(d):
        return lax.rem(gz + d, NZ)

    loads = []
    for s in range(S):
        for c, src in enumerate((k_hbm, v_hbm)):
            loads.append(
                pltpu.make_async_copy(
                    src.at[:, pl.ds(STARTS[s], STAGES[s])], kvb[s].at[:, c], kv_sem.at[2 * s + c]
                )
            )
    mine = pl.ds(ROWS * gz, ROWS)
    selfs = [
        pltpu.make_async_copy(k_hbm.at[mine], okv.at[:, gz, 0], self_sem.at[0]),
        pltpu.make_async_copy(v_hbm.at[mine], okv.at[:, gz, 1], self_sem.at[1]),
        pltpu.make_async_copy(q_hbm.at[mine], qb.at[:, gz], self_sem.at[2]),
    ]
    for cp in loads + selfs:
        cp.start()

    rqv[...] = jnp.zeros((NG, 1, 128), jnp.int32)

    bar = pltpu.get_barrier_semaphore()

    @pl.loop(1, NG)
    def _(s):
        pl.semaphore_signal(
            bar, 1, device_id=plane(lax.rem(g + s, NG)), device_id_type=MESH
        )

    for d in range(1, NZ):
        pl.semaphore_signal(bar, 1, device_id=(gx, gy, line(d)), device_id_type=MESH)

    owner_row = lax.broadcasted_iota(jnp.int32, (NG, 1, 128), 0)
    table = jnp.zeros((NG, 1, 128), jnp.int32)
    for b in range(BLOCKS):
        for j in range(2):
            e = ch[j, b]
            live = e >= 0
            o = jnp.where(live, lax.shift_right_logical(e, 3), -1)
            table = jnp.where(owner_row == o, lax.bitwise_and(e, 7) + 1, table)
    want[...] = table
    pl.semaphore_wait(bar, NG - 1 + NZ - 1)

    def ask(t, slot):
        return pltpu.make_async_remote_copy(
            src_ref=want.at[t], dst_ref=rqv.at[slot], send_sem=w_send.at[t],
            recv_sem=w_recv.at[slot], device_id=plane(t), device_id_type=MESH,
        )

    def sends_to(t):
        return (t > g) & (t >= 2)

    def gets_from(t):
        return (t < g) & (g >= 2)

    @pl.loop(0, NG)
    def _(t):
        @pl.when(gets_from(t))
        def _():
            ask(t, g).start()

    def ycopies(r, d):
        row, z, src_z = ROWS * line(d) + r, line(d), gz
        out = []
        for n, (src, dst) in enumerate(
            (
                (k_hbm.at[row], okv.at[r, src_z, 0]),
                (v_hbm.at[row], okv.at[r, src_z, 1]),
                (q_hbm.at[row], qb.at[r, src_z]),
            )
        ):
            out.append(
                pltpu.make_async_remote_copy(
                    src_ref=src, dst_ref=dst, send_sem=y_send.at[r, d - 1, n],
                    recv_sem=y_recv.at[r, d - 1, n], device_id=(gx, gy, z), device_id_type=MESH,
                )
            )
        return out

    DORDER = (2, 1, 3)
    for r in range(ROWS):
        for d in DORDER:
            for cp in ycopies(r, d):
                cp.start()

    for cp in loads:
        cp.wait()

    @pl.loop(0, NG)
    def _(t):
        @pl.when(sends_to(t))
        def _():
            ask(t, t).wait_recv()

    rq = pltpu.make_async_copy(rqv, rqs, rq_sem)
    rq.start()
    rq.wait()

    def give(s, t, slot):
        return pltpu.make_async_remote_copy(
            src_ref=stg[s].at[t], dst_ref=recv[s].at[slot], send_sem=a_send.at[s, t],
            recv_sem=a_recv.at[s, slot], device_id=plane(t), device_id_type=MESH,
        )

    def shifted(dz, dx, dc):
        return (
            lax.rem(gx + dz, NX) * NY + lax.rem(xx + dx, NXX) * 2 + lax.rem(cc + dc, 2)
        )

    def stage(s):
        @pl.loop(0, NG)
        def _(t):
            @pl.when(sends_to(t))
            def _():
                idx = jnp.maximum(rqs[t, 0, 0] - 1, 0)
                stg[s][t] = kvb[s][idx]

        recv[s][g] = kvb[s][0]

    def fire(s):
        def one(t):
            @pl.when(sends_to(t))
            def _():
                give(s, t, g).start()

        @pl.loop(0, 8)
        def _(i):
            one(shifted(i // 2, 2, lax.rem(i, 2)))

        @pl.loop(0, 16)
        def _(i):
            one(shifted(i // 4, 1 + 2 * lax.rem(i // 2, 2), lax.rem(i, 2)))

        @pl.loop(1, 8)
        def _(i):
            one(shifted(i // 2, 0, lax.rem(i, 2)))

    for s in range(S):
        stage(s)
        if s < AHEAD:
            fire(s)

    c2 = DH ** -0.5 * LOG2E

    def heads_of(r, qq, h):
        return qb[r, qq, :, h * DH : (h + 1) * DH]

    def scores_of(r, qq, h, keys):
        return lax.dot_general(
            heads_of(r, qq, h), keys, (((1,), (1,)), ((), ())),
            preferred_element_type=jnp.float32,
        )

    def weigh(p, values):
        ones = jnp.ones(values.shape, jnp.bfloat16)
        both = jnp.dot(
            p.astype(jnp.bfloat16), jnp.concatenate([values, ones], axis=1),
            preferred_element_type=jnp.float32,
        )
        return both[:, :DH], both[:, DH:]

    tok = lax.broadcasted_iota(jnp.int32, (QT, QT), 0)
    key_pos = lax.broadcasted_iota(jnp.int32, (QT, QT), 1)
    diag = key_pos <= tok

    def wide(x, n):
        return jnp.concatenate([x] * (n // DH), axis=1) if n > DH else x

    def pipeline(items):
        ready = items[0][0]()
        for n, (_, finish) in enumerate(items):
            ahead = items[n + 1][0]() if n + 1 < len(items) else None
            finish(ready)
            ready = ahead

    def peak(sc):
        return jnp.broadcast_to(jnp.max(sc, axis=1, keepdims=True), (QT, DH))

    def own_item(r, qq, h):
        n = qq + 1

        def first():
            return scores_of(r, qq, h, okv[r, 0:n, 0].reshape(n * QT, DH))

        def finish(sc):
            last = jnp.where(diag, sc[:, qq * QT :], NEG)
            sc = jnp.concatenate([sc[:, : qq * QT], last], axis=1) if qq else last
            top = peak(sc)
            p = jnp.exp2(sc * c2 - wide(top * c2, n * QT))
            pv, tot = weigh(p, okv[r, 0:n, 1].reshape(n * QT, DH))
            m_s[r, qq, h] = top
            l_s[r, qq, h] = tot
            acc[r, qq, h] = pv

        return first, finish

    def own(r):
        pipeline([own_item(r, qq, h) for qq in range(NZ) for h in range(HEADS)])

    def far_item(s, r, qq, h, live, last):
        n = 2 * NZ * STAGES[s]

        def first():
            return scores_of(r, qq, h, far[s][r, :, :, 0].reshape(n, DH))

        def finish(sc):
            old = m_s[r, qq, h]
            new = jnp.where(live, jnp.maximum(old, peak(sc)), old)
            base = jnp.where(live, new * c2, -NEG)
            p = jnp.exp2(sc * c2 - wide(base, n))
            fade = jnp.exp2((old - new) * c2)
            pv, tot = weigh(p, far[s][r, :, :, 1].reshape(n, DH))
            a_new = acc[r, qq, h] * fade + pv
            l_new = l_s[r, qq, h] * fade + tot
            if last:
                obuf[r, qq, :, h * DH : (h + 1) * DH] = (a_new / l_new).astype(jnp.bfloat16)
            else:
                m_s[r, qq, h] = new
                acc[r, qq, h] = a_new
                l_s[r, qq, h] = l_new

        return first, finish

    def extend(s, r, qqs, last):
        live = ch[0, ROWS * gz + r] >= 0
        pipeline([far_item(s, r, qq, h, live, last) for qq in qqs for h in range(HEADS)])

    def fcopy(s, r, d):
        return pltpu.make_async_remote_copy(
            src_ref=sel[s].at[r, d - 1], dst_ref=far[s].at[r, gz],
            send_sem=f_send.at[s, r, d - 1], recv_sem=f_recv.at[s, r, d - 1],
            device_id=(gx, gy, line(d)), device_id_type=MESH,
        )

    def forward(s):
        @pl.loop(0, NG)
        def _(t):
            @pl.when(gets_from(t))
            def _():
                give(s, t, t).wait_recv()

        if s + AHEAD < S:
            fire(s + AHEAD)

        for r in range(ROWS):
            for d in DORDER + (NZ,):
                for j in range(2):
                    e = ch[j, ROWS * line(d) + r]
                    o = jnp.where(e >= 0, lax.shift_right_logical(e, 3), g)
                    val = recv[s][o]
                    if d < NZ:
                        sel[s][r, d - 1, j] = val
                    else:
                        far[s][r, gz, j] = val
            for d in DORDER:
                fcopy(s, r, d).start()

    def wait_own(r):
        for d in DORDER:
            for cp in ycopies(r, d):
                cp.wait_recv()

    def wait_far(s, r):
        for d in DORDER:
            fcopy(s, r, d).wait_recv()

    for cp in selfs:
        cp.wait()
    wait_own(0)
    own(0)
    forward(0)
    wait_own(1)
    own(1)
    if S > 1:
        forward(1)
    for s in range(S - 1):
        for r in range(ROWS):
            wait_far(s, r)

            @pl.loop(0, NZ // PAIR)
            def _(i, s=s, r=r):
                extend(s, r, [PAIR * i + n for n in range(PAIR)], False)

        if s + 2 < S:
            forward(s + 2)

    def ocopy(r, d):
        return pltpu.make_async_remote_copy(
            src_ref=obuf.at[r, line(d)], dst_ref=out_ref.at[ROWS * gz + r],
            send_sem=o_send.at[r, d - 1], recv_sem=o_recv.at[r, d - 1],
            device_id=(gx, gy, line(d)), device_id_type=MESH,
        )

    for r in range(ROWS):
        wait_far(S - 1, r)

        @pl.loop(1, NZ + 1)
        def _(d, r=r):
            extend(S - 1, r, [lax.rem(gz + d, NZ)], True)

            @pl.when(d >= 2)
            def _():
                ocopy(r, d - 1).start()

        out_ref[ROWS * gz + r] = obuf[r, gz]

    @pl.loop(0, NG)
    def _(t):
        @pl.when(gets_from(t))
        def _():
            ask(t, g).wait_send()

    for r in range(ROWS):
        for d in range(1, NZ):
            for cp in ycopies(r, d):
                cp.wait_send()
            for s in range(S):
                fcopy(s, r, d).wait_send()
    for s in range(S):

        @pl.loop(0, NG)
        def _(t, s=s):
            @pl.when(sends_to(t))
            def _():
                give(s, t, g).wait_send()

    for r in range(ROWS):
        for d in range(1, NZ):
            ocopy(r, d).wait()


def body(queries, key_vectors, value_vectors, chosen):
    blocks, quarter, width = queries.shape
    dh = key_vectors.shape[2]
    heads = width // dh
    nx, ny, nz = (lax.axis_size(a) for a in ("gx", "gy", "gz"))
    rows = blocks // nz
    ng = nx * ny
    s = len(STAGES)
    bf, f32, i32 = jnp.bfloat16, jnp.float32, jnp.int32
    dma = pltpu.SemaphoreType.DMA
    scratch = [
        pltpu.VMEM((rows, nz, quarter, width), bf),
        pltpu.VMEM((rows, nz, 2, quarter, dh), bf),
        pltpu.VMEM((ng, 1, 128), i32),
        pltpu.VMEM((ng, 1, 128), i32),
        pltpu.SMEM((ng, 1, 128), i32),
        pltpu.VMEM((rows, nz, heads, quarter, dh), f32),
        pltpu.VMEM((rows, nz, heads, quarter, dh), f32),
        pltpu.VMEM((rows, nz, heads, quarter, dh), f32),
        pltpu.VMEM((rows, nz, quarter, width), bf),
        dma((2 * s,)),
        dma((3,)),
        dma((rows, nz - 1, 3)),
        dma((rows, nz - 1, 3)),
        dma((ng,)),
        dma((ng,)),
        dma,
        dma((s, ng)),
        dma((s, ng)),
        dma((s, rows, nz - 1)),
        dma((s, rows, nz - 1)),
        dma((rows, nz - 1)),
        dma((rows, nz - 1)),
    ]
    for lead in ((ng,), (ng,), (blocks,), (rows, nz - 1, 2), (rows, nz, 2)):
        scratch += [pltpu.VMEM(lead + (2, t, dh), bf) for t in STAGES]
    return pl.pallas_call(
        functools.partial(kernel, (nx, ny, nz, heads, dh, quarter, rows)),
        out_shape=pltpu.VMEM(queries.shape, bf),
        in_specs=[pl.BlockSpec(memory_space=pltpu.SMEM)]
        + [pl.BlockSpec(memory_space=pltpu.HBM)] * 3,
        out_specs=pl.BlockSpec(memory_space=pltpu.VMEM),
        scratch_shapes=scratch,
        compiler_params=pltpu.CompilerParams(
            collective_id=0, has_side_effects=True, vmem_limit_bytes=67043328 - 9 * 262144
        ),
    )(chosen.T, queries, key_vectors, value_vectors)


def solution(mesh):
    placed = (
        P(("gx", "gy"), "gz", None),
        P(("gx", "gy"), "gz", None),
        P(("gx", "gy"), "gz", None),
        P(("gx", "gy"), None),
    )
    return jax.shard_map(
        body, mesh=mesh, in_specs=placed, out_specs=P(("gx", "gy"), "gz", None), check_vma=False
    )
```
